8 devices in a mesh: dp: 1 (over z), tp: 2 (over y), cp: 4 (over x, core).
Axes of the slice: x: 2, y: 2, z: 1, core: 2. Of those that a mesh axis runs over, the one named last changes fastest.
Arguments:
- x: bfloat16 [4096, 2048], P(('dp', 'cp', 'tp'))
- w_q: bfloat16 [2048, 2048], P(None, 'tp')
- w_k: bfloat16 [2048, 256], P(None, 'tp')
- w_v: bfloat16 [2048, 256], P(None, 'tp')
- w_o: bfloat16 [2048, 2048], P('tp')
Outputs:
- output: bfloat16 [4096, 2048], P(('dp', 'cp', 'tp'))
All inputs are finite; a program needn't handle non-finite values.
Results may differ from the reference program's by a relative error of at most 0.00538824.
Values are sent between devices in bfloat16 or wider.
A program may use at most 1 GiB of HBM per device.

```python
import jax
import jax.numpy as jnp
from jax import lax

D = 2048
HEADS = 16
KV_HEADS = 2
HEAD = 128
SEQ = 4096
CP = 4
Q_BLOCK = 128


def stored_positions():
    piece_len = SEQ // (2 * CP)
    row_idx = jnp.arange(SEQ)
    block_idx = row_idx // (2 * piece_len)
    within = row_idx % (2 * piece_len)
    return jnp.where(within < piece_len, block_idx * piece_len + within, (2 * CP - 1 - block_idx) * piece_len + within - piece_len)


def setup_inputs(seed: int = 0, part: int = 0) -> dict:
    base_key = jax.random.key(seed)
    key_x = jax.random.fold_in(jax.random.fold_in(base_key, 1), part)
    key_q, key_k, key_v, key_o = jax.random.split(jax.random.fold_in(base_key, 2), 4)
    x_val = jax.random.normal(key_x, (SEQ, D), jnp.float32)
    w_q = jax.random.normal(key_q, (D, HEADS * HEAD), jnp.float32) * (1.6 * D ** -0.5)
    w_k = jax.random.normal(key_k, (D, KV_HEADS * HEAD), jnp.float32) * (1.6 * D ** -0.5)
    w_v = jax.random.normal(key_v, (D, KV_HEADS * HEAD), jnp.float32) * (D ** -0.5)
    w_o = jax.random.normal(key_o, (HEADS * HEAD, D), jnp.float32) * (3.0 * (HEADS * HEAD) ** -0.5)
    return {"x": x_val.astype(jnp.bfloat16), "w_q": w_q.astype(jnp.bfloat16), "w_k": w_k.astype(jnp.bfloat16), "w_v": w_v.astype(jnp.bfloat16), "w_o": w_o.astype(jnp.bfloat16)}


def reference(x, w_q, w_k, w_v, w_o):
    group_size = HEADS // KV_HEADS
    score_scale = HEAD ** -0.5
    q_proj = jnp.dot(x, w_q, preferred_element_type=jnp.float32).astype(jnp.bfloat16)
    k_proj = jnp.dot(x, w_k, preferred_element_type=jnp.float32).astype(jnp.bfloat16)
    v_proj = jnp.dot(x, w_v, preferred_element_type=jnp.float32).astype(jnp.bfloat16)
    q_blocks = q_proj.astype(jnp.float32).reshape(SEQ // Q_BLOCK, Q_BLOCK, KV_HEADS, group_size, HEAD)
    k_heads = jnp.transpose(k_proj.astype(jnp.float32).reshape(SEQ, KV_HEADS, HEAD), (1, 0, 2))
    v_heads = jnp.transpose(v_proj.astype(jnp.float32).reshape(SEQ, KV_HEADS, HEAD), (1, 0, 2))
    positions = stored_positions()
    pos_blocks = positions.reshape(SEQ // Q_BLOCK, Q_BLOCK)

    def one_block(block_args):
        q_blk, pos_blk = block_args
        visible = pos_blk[:, None] >= positions[None, :]

        def one_head(head_args):
            q_head, k_head, v_head = head_args
            scores = jnp.einsum("qge,ke->gqk", q_head, k_head) * score_scale
            scores = jnp.where(visible[None], scores, -jnp.inf)
            row_max = scores.max(axis=-1, keepdims=True)
            p_block = jnp.exp(scores - row_max)
            row_sum = p_block.sum(axis=-1)
            weighted = jnp.einsum("gqk,ke->qge", p_block.astype(jnp.bfloat16).astype(jnp.float32), v_head)
            return weighted / jnp.transpose(row_sum)[:, :, None]

        head_outs = lax.map(one_head, (jnp.transpose(q_blk, (1, 0, 2, 3)), k_heads, v_heads))
        return jnp.transpose(head_outs, (1, 0, 2, 3))

    attn_out = lax.map(one_block, (q_blocks, pos_blocks))
    attn_out = attn_out.reshape(SEQ, HEADS * HEAD).astype(jnp.bfloat16)
    return jnp.dot(attn_out, w_o, preferred_element_type=jnp.float32).astype(jnp.bfloat16)
```

```python
import functools

import jax
import jax.numpy as jnp
from jax import lax
from jax.experimental import pallas as pl
from jax.experimental.pallas import tpu as pltpu
from jax.sharding import PartitionSpec as P

HD = 128
R = 512
MESH = pl.DeviceIdType.MESH
F32 = jnp.float32
BF16 = jnp.bfloat16
EXP2_SCALE = (HD ** -0.5) * 1.4426950408889634
N_ITEMS = 13


def dot_nt(a, b):
    return lax.dot_general(a, b, (((1,), (1,)), ((), ())), preferred_element_type=F32)


def dot_nn(a, b):
    return jnp.dot(a, b, preferred_element_type=F32)


def kernel(x_hbm, wq_hbm, wk_hbm, wv_hbm, wo_hbm, out_ref,
           xs, wkv_n, wq_n, wo_n, a_f, wo_f, kvb, qb, ob, m_st, l_st, acc_st, yacc,
           lsem, ys, yr, xsnd, xr, d1s, d1r, d2s, d2r, kvr, kvs):
    dp = lax.axis_index("dp")
    tp = lax.axis_index("tp")
    cp = lax.axis_index("cp")
    xc = cp // 2
    core = cp % 2
    cp_sib = cp + 1 - 2 * core
    cp_x = (cp + 2) % 4
    cp_xs = (cp_sib + 2) % 4
    sib = (dp, tp, cp_sib)
    xn = (dp, tp, cp_x)
    yn = (dp, 1 - tp, cp)
    dg = (dp, 1 - tp, cp_x)
    far = 1 - tp

    def piece_of(c):
        return c + tp * (7 - 2 * c)

    p = piece_of(cp)
    p_sib = piece_of(cp_sib)
    p_x = piece_of(cp_x)
    p_xs = piece_of(cp_xs)
    is_h = tp == 1
    is_l = tp == 0
    x_sends = xc == tp
    x_gets = xc != tp

    def load(i, src, dst):
        return pltpu.make_async_copy(src, dst, lsem.at[i])

    loads = [load(0, x_hbm, xs),
             load(1, wk_hbm, wkv_n.at[:, pl.ds(0, HD)]),
             load(2, wv_hbm, wkv_n.at[:, pl.ds(HD, HD)])]
    loads += [load(3 + j, wq_hbm.at[:, pl.ds(256 * j, 256)], wq_n.at[j]) for j in range(4)]
    loads += [load(7, wo_hbm, wo_n)]
    for cpy in loads:
        cpy.start()

    bar = pltpu.get_barrier_semaphore()
    for dev in (sib, xn, yn, dg):
        pl.semaphore_signal(bar, 1, device_id=dev, device_id_type=MESH)
    pl.semaphore_wait(bar, 4)

    def remote(src, dst, ss, rs, dev):
        return pltpu.make_async_remote_copy(src, dst, ss, rs, device_id=dev, device_id_type=MESH)

    def quarter(k, q):
        if isinstance(k, int) and k == 0:
            return [a_f.at[0, pl.ds(q * 512, 512), :]]
        if isinstance(k, int) and k < 5:
            return [a_f.at[k, pl.ds(q * 512, 512), :]]
        return [wo_f.at[k - 5, pl.ds(q * 32, 32), :]]

    def y_send(k):
        q = cp
        if isinstance(k, int) and k == 0:
            rows = pl.ds(q * 512, 512)
            return [remote(wk_hbm.at[rows, :], a_f.at[0, rows, pl.ds(0, HD)], ys.at[0], yr.at[0], yn),
                    remote(wv_hbm.at[rows, :], a_f.at[0, rows, pl.ds(HD, HD)], ys.at[13], yr.at[13], yn)]
        if isinstance(k, int) and k < 5:
            rows = pl.ds(q * 512, 512)
            return [remote(wq_hbm.at[rows, pl.ds(256 * (k - 1), 256)], a_f.at[k, rows, :], ys.at[k], yr.at[k], yn)]
        return [remote(wo_hbm.at[pl.ds((k - 5) * HD + q * 32, 32), :], wo_f.at[k - 5, pl.ds(q * 32, 32), :],
                       ys.at[k], yr.at[k], yn)]

    def x_fwd(k):
        r = quarter(k, cp)[0]
        return remote(r, r, xsnd.at[k], xr.at[k], xn)

    def x_in(k):
        r = quarter(k, cp_x)[0]
        return remote(r, r, xsnd.at[k], xr.at[k], xn)

    def d1_fwd(k):
        r = quarter(k, cp)[0]
        return remote(r, r, d1s.at[k], d1r.at[k], sib)

    def d1_in(k):
        r = quarter(k, cp_sib)[0]
        return remote(r, r, d1s.at[k], d1r.at[k], sib)

    def d2_fwd(k):
        r = quarter(k, cp_x)[0]
        return remote(r, r, d2s.at[k], d2r.at[k], sib)

    def d2_in(k):
        r = quarter(k, cp_xs)[0]
        return remote(r, r, d2s.at[k], d2r.at[k], sib)

    def start_y(k):
        for c in y_send(k):
            c.start()

    def relay_y(k):
        for c in y_send(k):
            c.wait_recv()
        x_fwd(k).start()
        d1_fwd(k).start()

    def relay_x(k):
        x_in(k).wait_recv()
        d2_fwd(k).start()

    def ready(k):
        d1_in(k).wait_recv()
        d2_in(k).wait_recv()

    def kv_ref(piece, e):
        return kvb.at[e, pl.ds(piece * R, R), :]

    def kv_copy(piece, e, ssem, dev):
        r = kv_ref(piece, e)
        return remote(r, r, ssem, kvr.at[piece, e], dev)

    def kv_wait(piece, e):
        kv_copy(piece, e, kvs.at[0], sib).wait_recv()

    def own_kv_sends(e, slot, diag):
        kv_copy(p, e, kvs.at[slot], sib).start()

        @pl.when(x_sends)
        def _():
            kv_copy(p, e, kvs.at[2 + slot], xn).start()

        @pl.when(is_l)
        def _():
            kv_copy(p, e, kvs.at[4 + slot], yn).start()
            if diag:
                kv_copy(p, e, kvs.at[6], dg).start()

    def project(w):
        return dot_nn(xs[...], w).astype(BF16)

    def kv_project(w, e):
        kvb[e, pl.ds(pl.multiple_of(p * R, R), R), :] = project(w)

    def soft_new(h, rows, s, v):
        m = jnp.max(s, axis=-1, keepdims=True)
        pr = jnp.exp2((s - m) * EXP2_SCALE)
        n = s.shape[1]
        l = pr[:, 0:128]
        for t in range(1, n // 128):
            l = l + pr[:, t * 128:(t + 1) * 128]
        m_st[h, rows, :] = jnp.broadcast_to(m, (m.shape[0], 128))
        l_st[h, rows, :] = l
        acc_st[h, rows, :] = dot_nn(pr.astype(BF16), v)

    def soft_add(h, rows, s, v):
        m_old = m_st[h, rows, :]
        m_new = jnp.maximum(m_old, jnp.max(s, axis=-1, keepdims=True))
        alpha = jnp.exp2((m_old - m_new) * EXP2_SCALE)
        n = s.shape[1]
        parts = [jnp.exp2((s[:, t * 128:(t + 1) * 128] - m_new) * EXP2_SCALE) for t in range(n // 128)]
        l = parts[0]
        for t in range(1, n // 128):
            l = l + parts[t]
        pr = jnp.concatenate(parts, axis=1)
        m_st[h, rows, :] = m_new
        l_st[h, rows, :] = l_st[h, rows, :] * alpha + l
        acc_st[h, rows, :] = acc_st[h, rows, :] * alpha + dot_nn(pr.astype(BF16), v)

    def att_self(h, qi, e):
        base = pl.multiple_of(p * R, R)
        k_lo = kvb[e, pl.ds(base, 256), 0:HD]
        v_lo = kvb[e, pl.ds(base, 256), HD:2 * HD]
        k_all = kvb[e, pl.ds(base, R), 0:HD]
        v_all = kvb[e, pl.ds(base, R), HD:2 * HD]
        row = lax.broadcasted_iota(jnp.int32, (256, 256), 0)
        col = lax.broadcasted_iota(jnp.int32, (256, 256), 1)
        s = dot_nt(qb[qi, 0:256, :], k_lo)
        soft_new(h, slice(0, 256), jnp.where(row >= col, s, -jnp.inf), v_lo)
        row2 = lax.broadcasted_iota(jnp.int32, (256, 512), 0) + 256
        col2 = lax.broadcasted_iota(jnp.int32, (256, 512), 1)
        s = dot_nt(qb[qi, 256:512, :], k_all)
        soft_new(h, slice(256, 512), jnp.where(row2 >= col2, s, -jnp.inf), v_all)

    def att_piece(h, qi, e, piece):
        base = pl.multiple_of(piece * R, R)
        k = kvb[e, pl.ds(base, R), 0:HD]
        v = kvb[e, pl.ds(base, R), HD:2 * HD]
        for c in range(2):
            rows = slice(256 * c, 256 * c + 256)
            soft_add(h, rows, dot_nt(qb[qi, rows, :], k), v)

    def finish_head(h, oi):
        l = jnp.sum(l_st[h], axis=-1, keepdims=True)
        ob[oi] = (acc_st[h] / l).astype(BF16)

    start_y(0)
    start_y(1)
    loads[0].wait()
    loads[1].wait()
    loads[2].wait()
    kv_project(wkv_n[...], tp)
    own_kv_sends(tp, 0, False)

    for j in range(4):
        loads[3 + j].wait()

    def q_near(j, carry):
        r = project(wq_n[j])
        qb[2 * j] = r[:, 0:HD]
        qb[2 * j + 1] = r[:, HD:2 * HD]
        return carry

    lax.fori_loop(0, 4, q_near, 0)

    def near_self(h, carry):
        att_self(h, h, tp)
        return carry

    lax.fori_loop(0, 8, near_self, 0)

    relay_y(0)
    start_y(2)

    kv_wait(p_sib, tp)

    def near_range(lo, hi):
        n = hi - lo

        def body(i, carry):
            att_piece(i // n, i // n, tp, lo + i % n)
            return carry

        lax.fori_loop(0, 8 * n, body, 0)

    @pl.when(p_sib < p)
    def _():
        def body(h, carry):
            att_piece(h, h, tp, p_sib)
            return carry

        lax.fori_loop(0, 8, body, 0)

    relay_y(1)
    start_y(3)
    relay_x(0)

    @pl.when(x_gets)
    def _():
        kv_wait(p_x, tp)
        kv_copy(p_x, tp, kvs.at[7], sib).start()
        kv_wait(p_xs, tp)

        def body(i, carry):
            att_piece(i // 2, i // 2, tp, lax.min(p_x, p_xs) + i % 2)
            return carry

        lax.fori_loop(0, 16, body, 0)

    ready(0)
    kv_project(a_f[0], far)
    own_kv_sends(far, 1, True)

    relay_y(2)
    start_y(4)
    relay_x(1)

    @pl.when(is_h)
    def _():
        kv_wait(cp, 0)
        kv_copy(cp, 0, kvs.at[11], xn).start()
        kv_copy(cp, 0, kvs.at[9], sib).start()
        kv_wait(cp_x, 0)
        kv_copy(cp_x, 0, kvs.at[12], sib).start()

    @pl.when(x_gets)
    def _():
        kv_wait(p_x, far)
        kv_copy(p_x, far, kvs.at[8], sib).start()

    kv_wait(p_sib, far)

    @pl.when(x_gets)
    def _():
        kv_wait(p_xs, far)

    @pl.when(is_h)
    def _():
        kv_wait(cp_sib, 0)
        kv_wait(cp_xs, 0)

    def far_q(j):
        r = project(a_f[1 + j])
        qb[8 + 2 * j] = r[:, 0:HD]
        qb[9 + 2 * j] = r[:, HD:2 * HD]

    def far_head(hf):
        att_self(hf, 8 + hf, far)

        def body(i, carry):
            att_piece(hf, 8 + hf, far, i)
            return carry

        lax.fori_loop(0, p, body, 0)
        finish_head(hf, 8 + hf)

    def far_head_slot(hf, slot):
        att_self(slot, 8 + hf, far)

        def body(i, carry):
            att_piece(slot, 8 + hf, far, i)
            return carry

        lax.fori_loop(0, p, body, 0)
        finish_head(slot, 8 + hf)

    ready(1)
    far_q(0)

    def far0(i, carry):
        far_head_slot(i, 8 + i % 2)
        return carry

    lax.fori_loop(0, 2, far0, 0)

    relay_y(3)
    start_y(5)
    start_y(6)
    relay_x(2)

    @pl.when(is_h)
    def _():
        kv_wait(cp, 1)
        kv_copy(cp, 1, kvs.at[10], sib).start()
        kv_wait(cp_x, 1)
        kv_copy(cp_x, 1, kvs.at[13], sib).start()
        kv_wait(cp_sib, 1)
        kv_wait(cp_xs, 1)

        def body(i, carry):
            att_piece(i // 4, i // 4, 1, i % 4)
            return carry

        lax.fori_loop(0, 16, body, 0)

    relay_y(4)
    start_y(7)
    start_y(8)
    relay_x(3)

    @pl.when(is_h)
    def _():
        def body(i, carry):
            att_piece(i // 4, i // 4, 1, i % 4)
            return carry

        lax.fori_loop(16, 32, body, 0)

    def near_finish(h, carry):
        finish_head(h, h)
        return carry

    lax.fori_loop(0, 8, near_finish, 0)

    loads[7].wait()

    def near_out(t, carry):
        cols = pl.ds(pl.multiple_of(t * 512, 512), 512)
        o_all = jnp.concatenate([ob[i] for i in range(8)], axis=1)
        yacc[:, cols] = dot_nn(o_all, wo_n[:, cols])
        return carry

    lax.fori_loop(0, 4, near_out, 0)

    def far_rest(i, carry):
        hf = i + 2

        @pl.when(i == 0)
        def _():
            relay_x(4)

        @pl.when(i > 0)
        def _():
            relay_x(4 + i)

        relay_y(5 + i)

        @pl.when(i < 4)
        def _():
            start_y(9 + i)

        @pl.when(i % 2 == 0)
        def _():
            j = hf // 2
            rd = a_f.at[1 + j, pl.ds(cp_sib * 512, 512), :]
            remote(rd, rd, d1s.at[1 + j], d1r.at[1 + j], sib).wait_recv()
            rd2 = a_f.at[1 + j, pl.ds(cp_xs * 512, 512), :]
            remote(rd2, rd2, d2s.at[1 + j], d2r.at[1 + j], sib).wait_recv()
            far_q(j)

        far_head_slot(hf, 8 + i % 2)
        return carry

    lax.fori_loop(0, 6, far_rest, 0)

    def far_out(j, last):
        ready(5 + 2 * j)
        ready(6 + 2 * j)

        def body(t, carry):
            cols = pl.ds(pl.multiple_of(t * 512, 512), 512)
            o_pair = jnp.concatenate([ob[8 + 2 * j], ob[9 + 2 * j]], axis=1)
            w = jnp.concatenate([wo_f[2 * j, :, cols], wo_f[2 * j + 1, :, cols]], axis=0)
            r = yacc[:, cols] + dot_nn(o_pair, w)
            if last:
                out_ref[:, cols] = r.astype(BF16)
            else:
                yacc[:, cols] = r
            return carry

        lax.fori_loop(0, 4, body, 0)

    relay_y(11)
    relay_x(10)
    far_out(0, False)
    relay_y(12)
    relay_x(11)
    far_out(1, False)
    relay_x(12)
    far_out(2, False)
    far_out(3, True)

    for k in range(5):
        for c in y_send(k):
            c.wait_send()
        x_fwd(k).wait_send()
        d1_fwd(k).wait_send()
        d2_fwd(k).wait_send()

    def drain(k, carry):
        for c in y_send(k):
            c.wait_send()
        x_fwd(k).wait_send()
        d1_fwd(k).wait_send()
        d2_fwd(k).wait_send()
        return carry

    lax.fori_loop(5, N_ITEMS, drain, 0)

    def sent(piece, e, slot, dev):
        kv_copy(piece, e, kvs.at[slot], dev).wait_send()

    sent(p, tp, 0, sib)
    sent(p, far, 1, sib)

    @pl.when(x_sends)
    def _():
        sent(p, tp, 2, xn)
        sent(p, far, 3, xn)

    @pl.when(x_gets)
    def _():
        sent(p_x, tp, 7, sib)
        sent(p_x, far, 8, sib)

    @pl.when(is_l)
    def _():
        sent(p, tp, 4, yn)
        sent(p, far, 5, yn)
        sent(p, far, 6, dg)

    @pl.when(is_h)
    def _():
        sent(cp, 0, 9, sib)
        sent(cp, 1, 10, sib)
        sent(cp, 0, 11, xn)
        sent(cp_x, 0, 12, sib)
        sent(cp_x, 1, 13, sib)


def solution(mesh):
    row_spec = P(("dp", "cp", "tp"), None)

    def local_layer(x_loc, w_q, w_k, w_v, w_o):
        anyspec = pl.BlockSpec(memory_space=pl.ANY)
        dma = pltpu.SemaphoreType.DMA
        return pl.pallas_call(
            kernel,
            out_shape=jax.ShapeDtypeStruct((R, 2048), BF16),
            in_specs=[anyspec] * 5,
            out_specs=pl.BlockSpec(memory_space=pltpu.VMEM),
            scratch_shapes=[
                pltpu.VMEM((R, 2048), BF16),
                pltpu.VMEM((2048, 256), BF16),
                pltpu.VMEM((4, 2048, 256), BF16),
                pltpu.VMEM((1024, 2048), BF16),
                pltpu.VMEM((5, 2048, 256), BF16),
                pltpu.VMEM((8, 128, 2048), BF16),
                pltpu.VMEM((2, 4096, 256), BF16),
                pltpu.VMEM((16, R, HD), BF16),
                pltpu.VMEM((16, R, HD), BF16),
                pltpu.VMEM((10, R, 128), F32),
                pltpu.VMEM((10, R, 128), F32),
                pltpu.VMEM((10, R, 128), F32),
                pltpu.VMEM((R, 2048), F32),
                dma((8,)),
                dma((14,)), dma((14,)),
                dma((13,)), dma((13,)),
                dma((13,)), dma((13,)),
                dma((13,)), dma((13,)),
                dma((8, 2)), dma((14,)),
            ],
            compiler_params=pltpu.CompilerParams(
                collective_id=0, has_side_effects=True, vmem_limit_bytes=62 * 1024 * 1024),
            name="attn_all",
        )(x_loc, w_q, w_k, w_v, w_o)

    return jax.shard_map(local_layer, mesh=mesh,
                         in_specs=(row_spec, P(None, "tp"), P(None, "tp"), P(None, "tp"), P("tp", None)),
                         out_specs=row_spec, check_vma=False)
```

```python
import functools

import jax
import jax.numpy as jnp
from jax import lax
from jax.experimental import pallas as pl
from jax.experimental.pallas import tpu as pltpu
from jax.sharding import PartitionSpec as P

HD = 128
R = 512
MESH = pl.DeviceIdType.MESH
F32 = jnp.float32
BF16 = jnp.bfloat16
EXP2_SCALE = (HD ** -0.5) * 1.4426950408889634
N_ITEMS = 13


def dot_nt(a, b):
    return lax.dot_general(a, b, (((1,), (1,)), ((), ())), preferred_element_type=F32)


def dot_nn(a, b):
    return jnp.dot(a, b, preferred_element_type=F32)


def kernel(x_hbm, wq_hbm, wk_hbm, wv_hbm, wo_hbm, out_ref,
           xs, wkv_n, wq_n, wo_n, a_f, wo_f, kvb, qb, ob, m_st, l_st, acc_st, yacc,
           lsem, ys, yr, xsnd, xr, d1s, d1r, d2s, d2r, kvr, kvs):
    dp = lax.axis_index("dp")
    tp = lax.axis_index("tp")
    cp = lax.axis_index("cp")
    xc = cp // 2
    core = cp % 2
    cp_sib = cp + 1 - 2 * core
    cp_x = (cp + 2) % 4
    cp_xs = (cp_sib + 2) % 4
    sib = (dp, tp, cp_sib)
    xn = (dp, tp, cp_x)
    yn = (dp, 1 - tp, cp)
    dg = (dp, 1 - tp, cp_x)
    far = 1 - tp

    def piece_of(c):
        return c + tp * (7 - 2 * c)

    p = piece_of(cp)
    p_sib = piece_of(cp_sib)
    p_x = piece_of(cp_x)
    p_xs = piece_of(cp_xs)
    is_h = tp == 1
    is_l = tp == 0
    x_sends = xc == tp
    x_gets = xc != tp

    def load(i, src, dst):
        return pltpu.make_async_copy(src, dst, lsem.at[i])

    loads = [load(0, x_hbm, xs),
             load(1, wk_hbm, wkv_n.at[:, pl.ds(0, HD)]),
             load(2, wv_hbm, wkv_n.at[:, pl.ds(HD, HD)])]
    loads += [load(3 + j, wq_hbm.at[:, pl.ds(256 * j, 256)], wq_n.at[j]) for j in range(4)]
    loads += [load(7, wo_hbm, wo_n)]
    for cpy in loads:
        cpy.start()

    bar = pltpu.get_barrier_semaphore()
    for dev in (sib, xn, yn, dg):
        pl.semaphore_signal(bar, 1, device_id=dev, device_id_type=MESH)
    pl.semaphore_wait(bar, 4)

    def remote(src, dst, ss, rs, dev):
        return pltpu.make_async_remote_copy(src, dst, ss, rs, device_id=dev, device_id_type=MESH)

    def quarter(k, q):
        if isinstance(k, int) and k == 0:
            return [a_f.at[0, pl.ds(q * 512, 512), :]]
        if isinstance(k, int) and k < 5:
            return [a_f.at[k, pl.ds(q * 512, 512), :]]
        return [wo_f.at[k - 5, pl.ds(q * 32, 32), :]]

    def y_send(k):
        q = cp
        if isinstance(k, int) and k == 0:
            rows = pl.ds(q * 512, 512)
            return [remote(wk_hbm.at[rows, :], a_f.at[0, rows, pl.ds(0, HD)], ys.at[0], yr.at[0], yn),
                    remote(wv_hbm.at[rows, :], a_f.at[0, rows, pl.ds(HD, HD)], ys.at[13], yr.at[13], yn)]
        if isinstance(k, int) and k < 5:
            rows = pl.ds(q * 512, 512)
            return [remote(wq_hbm.at[rows, pl.ds(256 * (k - 1), 256)], a_f.at[k, rows, :], ys.at[k], yr.at[k], yn)]
        return [remote(wo_hbm.at[pl.ds((k - 5) * HD + q * 32, 32), :], wo_f.at[k - 5, pl.ds(q * 32, 32), :],
                       ys.at[k], yr.at[k], yn)]

    def x_fwd(k):
        r = quarter(k, cp)[0]
        return remote(r, r, xsnd.at[k], xr.at[k], xn)

    def x_in(k):
        r = quarter(k, cp_x)[0]
        return remote(r, r, xsnd.at[k], xr.at[k], xn)

    def d1_fwd(k):
        r = quarter(k, cp)[0]
        return remote(r, r, d1s.at[k], d1r.at[k], sib)

    def d1_in(k):
        r = quarter(k, cp_sib)[0]
        return remote(r, r, d1s.at[k], d1r.at[k], sib)

    def d2_fwd(k):
        r = quarter(k, cp_x)[0]
        return remote(r, r, d2s.at[k], d2r.at[k], sib)

    def d2_in(k):
        r = quarter(k, cp_xs)[0]
        return remote(r, r, d2s.at[k], d2r.at[k], sib)

    def start_y(k):
        for c in y_send(k):
            c.start()

    def relay_y(k):
        for c in y_send(k):
            c.wait_recv()
        x_fwd(k).start()
        d1_fwd(k).start()

    def relay_x(k):
        x_in(k).wait_recv()
        d2_fwd(k).start()

    def ready(k):
        d1_in(k).wait_recv()
        d2_in(k).wait_recv()

    def kv_ref(piece, e):
        return kvb.at[e, pl.ds(piece * R, R), :]

    def kv_copy(piece, e, ssem, dev):
        r = kv_ref(piece, e)
        return remote(r, r, ssem, kvr.at[piece, e], dev)

    def kv_wait(piece, e):
        kv_copy(piece, e, kvs.at[0], sib).wait_recv()

    def own_kv_sends(e, slot, diag):
        kv_copy(p, e, kvs.at[slot], sib).start()

        @pl.when(x_sends)
        def _():
            kv_copy(p, e, kvs.at[2 + slot], xn).start()

        @pl.when(is_l)
        def _():
            kv_copy(p, e, kvs.at[4 + slot], yn).start()
            if diag:
                kv_copy(p, e, kvs.at[6], dg).start()

    def project(w):
        return dot_nn(xs[...], w).astype(BF16)

    def kv_project(w, e):
        kvb[e, pl.ds(pl.multiple_of(p * R, R), R), :] = project(w)

    def exp_scaled(d):
        return jnp.exp2(d * EXP2_SCALE)

    def soft_new(slot, rows, s, v):
        m = jnp.max(s, axis=-1, keepdims=True)
        parts = [exp_scaled(s[:, t:t + 128] - m) for t in range(0, s.shape[1], 128)]
        m_st[slot, rows, :] = jnp.broadcast_to(m, (m.shape[0], 128))
        l_st[slot, rows, :] = functools.reduce(jnp.add, parts)
        acc_st[slot, rows, :] = dot_nn(jnp.concatenate([t.astype(BF16) for t in parts], axis=1), v)

    def soft_add(slot, s, v):
        m_old = m_st[slot]
        m_new = jnp.maximum(m_old, jnp.max(s, axis=-1, keepdims=True))
        alpha = exp_scaled(m_old - m_new)
        parts = [exp_scaled(s[:, t:t + 128] - m_new) for t in range(0, s.shape[1], 128)]
        m_st[slot] = m_new
        l_st[slot] = l_st[slot] * alpha + functools.reduce(jnp.add, parts)
        pr = jnp.concatenate([t.astype(BF16) for t in parts], axis=1)
        acc_st[slot] = acc_st[slot] * alpha + dot_nn(pr, v)

    def att_self(slot, qi, e):
        base = pl.multiple_of(p * R, R)
        k = kvb[e, pl.ds(base, R), 0:HD]
        v = kvb[e, pl.ds(base, R), HD:2 * HD]
        row = lax.broadcasted_iota(jnp.int32, (256, 256), 0)
        col = lax.broadcasted_iota(jnp.int32, (256, 256), 1)
        s = dot_nt(qb[qi, 0:256, :], k[0:256])
        soft_new(slot, slice(0, 256), jnp.where(row >= col, s, -jnp.inf), v[0:256])
        row2 = lax.broadcasted_iota(jnp.int32, (256, 512), 0) + 256
        col2 = lax.broadcasted_iota(jnp.int32, (256, 512), 1)
        s = dot_nt(qb[qi, 256:512, :], k)
        soft_new(slot, slice(256, 512), jnp.where(row2 >= col2, s, -jnp.inf), v)

    def att_tile(slot, qi, e, piece, n_pieces):
        base = pl.multiple_of(piece * R, R)
        k = kvb[e, pl.ds(base, n_pieces * R), 0:HD]
        v = kvb[e, pl.ds(base, n_pieces * R), HD:2 * HD]
        for u in range(2):
            soft_add(slot + u, dot_nt(qb[qi + u], k), v)

    def finish_head(slot, oi):
        l = jnp.sum(l_st[slot], axis=-1, keepdims=True)
        ob[oi] = (acc_st[slot] / l).astype(BF16)

    def dyn(k, fn):
        @pl.when(k < 5)
        def _():
            fn(k, lambda q: a_f.at[k, pl.ds(q * 512, 512), :])

        @pl.when(k >= 5)
        def _():
            fn(k, lambda q: wo_f.at[k - 5, pl.ds(q * 32, 32), :])

    def ry(k):
        def fn(k, at):
            r = at(cp)
            remote(r, r, ys.at[k], yr.at[k], yn).wait_recv()
            remote(r, r, xsnd.at[k], xr.at[k], xn).start()
            remote(r, r, d1s.at[k], d1r.at[k], sib).start()
        dyn(k, fn)

    def rx(k):
        def fn(k, at):
            r = at(cp_x)
            remote(r, r, xsnd.at[k], xr.at[k], xn).wait_recv()
            remote(r, r, d2s.at[k], d2r.at[k], sib).start()
        dyn(k, fn)

    start_y(0)
    loads[0].wait()
    loads[1].wait()
    loads[2].wait()
    kv_project(wkv_n[...], tp)
    own_kv_sends(tp, 0, False)
    start_y(1)
    start_y(2)

    for j in range(4):
        loads[3 + j].wait()

    def q_near(j, carry):
        r = project(wq_n[j])
        qb[2 * j] = r[:, 0:HD]
        qb[2 * j + 1] = r[:, HD:2 * HD]
        return carry

    lax.fori_loop(0, 4, q_near, 0)

    def near_self(i, carry):
        att_self(2 * i, 2 * i, tp)
        att_self(2 * i + 1, 2 * i + 1, tp)
        return carry

    lax.fori_loop(0, 4, near_self, 0)

    relay_y(0)
    kv_wait(p_sib, tp)

    @pl.when(p_sib < p)
    def _():
        def body(i, carry):
            att_tile(2 * i, 2 * i, tp, p_sib, 1)
            return carry

        lax.fori_loop(0, 4, body, 0)

    @pl.when(is_h)
    def _():
        kv_wait(cp, 0)
        kv_copy(cp, 0, kvs.at[11], xn).start()
        kv_copy(cp, 0, kvs.at[9], sib).start()

    relay_x(0)

    @pl.when(x_gets)
    def _():
        kv_wait(p_x, tp)
        kv_copy(p_x, tp, kvs.at[7], sib).start()
        kv_wait(p_xs, tp)

        def body(i, carry):
            att_tile(2 * i, 2 * i, tp, lax.min(p_x, p_xs), 2)
            return carry

        lax.fori_loop(0, 4, body, 0)

    ready(0)
    kv_project(a_f[0], far)
    own_kv_sends(far, 1, True)
    for k in range(3, 5):
        start_y(k)

    def send_rest(k, carry):
        start_y(k)
        return carry

    lax.fori_loop(5, N_ITEMS, send_rest, 0)
    relay_y(1)

    @pl.when(is_h)
    def _():
        kv_wait(cp_x, 0)
        kv_copy(cp_x, 0, kvs.at[12], sib).start()

    @pl.when(x_gets)
    def _():
        kv_wait(p_x, far)
        kv_copy(p_x, far, kvs.at[8], sib).start()

    relay_y(2)
    relay_x(1)

    kv_wait(p_sib, far)

    @pl.when(x_gets)
    def _():
        kv_wait(p_xs, far)

    @pl.when(is_h)
    def _():
        kv_wait(cp_sib, 0)
        kv_wait(cp_xs, 0)

    def far_pair(j, carry):
        @pl.when(j == 2)
        def _():
            def body(i, c):
                @pl.when(is_h)
                def _():
                    att_tile(2 * i, 2 * i, 1, 0, 4)

                @pl.when(i < 3)
                def _():
                    ry(3 + i)

                @pl.when(i > 0)
                def _():
                    rx(2 + i)

                return c

            lax.fori_loop(0, 4, body, 0)

        rd = a_f.at[1 + j, pl.ds(cp_sib * 512, 512), :]
        remote(rd, rd, d1s.at[1 + j], d1r.at[1 + j], sib).wait_recv()
        rd2 = a_f.at[1 + j, pl.ds(cp_xs * 512, 512), :]
        remote(rd2, rd2, d2s.at[1 + j], d2r.at[1 + j], sib).wait_recv()
        r = project(a_f[1 + j])
        qi = 8 + 2 * j
        qb[qi] = r[:, 0:HD]
        qb[qi + 1] = r[:, HD:2 * HD]
        att_self(8, qi, far)
        att_self(9, qi + 1, far)

        @pl.when(j >= 2)
        def _():
            ry(3 * j)

        @pl.when(is_h)
        def _():
            att_tile(8, qi, far, 0, 4)

        @pl.when(j == 0)
        def _():
            rx(2)

        @pl.when(j == 1)
        def _():
            @pl.when(is_h)
            def _():
                kv_wait(cp, 1)
                kv_copy(cp, 1, kvs.at[10], sib).start()
                kv_wait(cp_x, 1)
                kv_copy(cp_x, 1, kvs.at[13], sib).start()
                kv_wait(cp_sib, 1)
                kv_wait(cp_xs, 1)

        @pl.when(j >= 2)
        def _():
            ry(3 * j + 1)
            rx(3 * j)

        lo = 4 * tp

        @pl.when(p - lo >= 2)
        def _():
            att_tile(8, qi, far, lo, 2)

        @pl.when((p - lo) % 2 == 1)
        def _():
            att_tile(8, qi, far, p - 1, 1)

        @pl.when(j >= 2)
        def _():
            rx(3 * j + 1)
            ry(3 * j + 2)

        finish_head(8, qi)
        finish_head(9, qi + 1)
        return carry

    lax.fori_loop(0, 4, far_pair, 0)

    relay_y(12)
    relay_x(8)
    relay_x(11)

    def near_finish(h, carry):
        finish_head(h, h)
        return carry

    lax.fori_loop(0, 8, near_finish, 0)

    loads[7].wait()

    def near_out(t, carry):
        cols = pl.ds(pl.multiple_of(t * 512, 512), 512)
        o_all = jnp.concatenate([ob[i] for i in range(8)], axis=1)
        yacc[:, cols] = dot_nn(o_all, wo_n[:, cols])
        return carry

    lax.fori_loop(0, 4, near_out, 0)

    def far_out(j, n, last):
        for k in range(2 * j, 2 * j + 2 * n):
            ready(5 + k)

        def body(t, carry):
            cols = pl.ds(pl.multiple_of(t * 512, 512), 512)
            o_pair = jnp.concatenate([ob[8 + k] for k in range(2 * j, 2 * j + 2 * n)], axis=1)
            w = jnp.concatenate([wo_f[k, :, cols] for k in range(2 * j, 2 * j + 2 * n)], axis=0)
            r = yacc[:, cols] + dot_nn(o_pair, w)
            if last:
                out_ref[:, cols] = r.astype(BF16)
            else:
                yacc[:, cols] = r
            return carry

        lax.fori_loop(0, 4, body, 0)

    far_out(0, 2, False)
    relay_x(12)
    far_out(2, 1, False)
    far_out(3, 1, True)

    for k in range(5):
        for c in y_send(k):
            c.wait_send()
        x_fwd(k).wait_send()
        d1_fwd(k).wait_send()
        d2_fwd(k).wait_send()

    def drain(k, carry):
        for c in y_send(k):
            c.wait_send()
        x_fwd(k).wait_send()
        d1_fwd(k).wait_send()
        d2_fwd(k).wait_send()
        return carry

    lax.fori_loop(5, N_ITEMS, drain, 0)

    def sent(piece, e, slot, dev):
        kv_copy(piece, e, kvs.at[slot], dev).wait_send()

    sent(p, tp, 0, sib)
    sent(p, far, 1, sib)

    @pl.when(x_sends)
    def _():
        sent(p, tp, 2, xn)
        sent(p, far, 3, xn)

    @pl.when(x_gets)
    def _():
        sent(p_x, tp, 7, sib)
        sent(p_x, far, 8, sib)

    @pl.when(is_l)
    def _():
        sent(p, tp, 4, yn)
        sent(p, far, 5, yn)
        sent(p, far, 6, dg)

    @pl.when(is_h)
    def _():
        sent(cp, 0, 9, sib)
        sent(cp, 1, 10, sib)
        sent(cp, 0, 11, xn)
        sent(cp_x, 0, 12, sib)
        sent(cp_x, 1, 13, sib)


def solution(mesh):
    row_spec = P(("dp", "cp", "tp"), None)

    def local_layer(x_loc, w_q, w_k, w_v, w_o):
        anyspec = pl.BlockSpec(memory_space=pl.ANY)
        dma = pltpu.SemaphoreType.DMA
        return pl.pallas_call(
            kernel,
            out_shape=jax.ShapeDtypeStruct((R, 2048), BF16),
            in_specs=[anyspec] * 5,
            out_specs=pl.BlockSpec(memory_space=pltpu.VMEM),
            scratch_shapes=[
                pltpu.VMEM((R, 2048), BF16),
                pltpu.VMEM((2048, 256), BF16),
                pltpu.VMEM((4, 2048, 256), BF16),
                pltpu.VMEM((1024, 2048), BF16),
                pltpu.VMEM((5, 2048, 256), BF16),
                pltpu.VMEM((8, 128, 2048), BF16),
                pltpu.VMEM((2, 4096, 256), BF16),
                pltpu.VMEM((16, R, HD), BF16),
                pltpu.VMEM((16, R, HD), BF16),
                pltpu.VMEM((10, R, 128), F32),
                pltpu.VMEM((10, R, 128), F32),
                pltpu.VMEM((10, R, 128), F32),
                pltpu.VMEM((R, 2048), F32),
                dma((8,)),
                dma((14,)), dma((14,)),
                dma((13,)), dma((13,)),
                dma((13,)), dma((13,)),
                dma((13,)), dma((13,)),
                dma((8, 2)), dma((14,)),
            ],
            compiler_params=pltpu.CompilerParams(
                collective_id=0, has_side_effects=True, vmem_limit_bytes=62 * 1024 * 1024),
            name="attn_all",
        )(x_loc, w_q, w_k, w_v, w_o)

    return jax.shard_map(local_layer, mesh=mesh,
                         in_specs=(row_spec, P(None, "tp"), P(None, "tp"), P(None, "tp"), P("tp", None)),
                         out_specs=row_spec, check_vma=False)
```

```python
import functools

import jax
import jax.numpy as jnp
from jax import lax
from jax.experimental import pallas as pl
from jax.experimental.pallas import tpu as pltpu
from jax.sharding import PartitionSpec as P

HD = 128
R = 512
MESH = pl.DeviceIdType.MESH
F32 = jnp.float32
BF16 = jnp.bfloat16
EXP2_SCALE = (HD ** -0.5) * 1.4426950408889634
N_ITEMS = 13


def dot_nt(a, b):
    return lax.dot_general(a, b, (((1,), (1,)), ((), ())), preferred_element_type=F32)


def dot_nn(a, b):
    return jnp.dot(a, b, preferred_element_type=F32)


def kernel(x_hbm, wq_hbm, wk_hbm, wv_hbm, wo_hbm, out_ref,
           xs, wkv_n, wq_n, wo_n, a_f, wo_f, kvb, qb, ob, m_st, l_st, acc_st, yacc,
           lsem, ys, yr, xsnd, xr, d1s, d1r, d2s, d2r, kvr, kvs):
    dp = lax.axis_index("dp")
    tp = lax.axis_index("tp")
    cp = lax.axis_index("cp")
    xc = cp // 2
    core = cp % 2
    cp_sib = cp + 1 - 2 * core
    cp_x = (cp + 2) % 4
    cp_xs = (cp_sib + 2) % 4
    sib = (dp, tp, cp_sib)
    xn = (dp, tp, cp_x)
    yn = (dp, 1 - tp, cp)
    dg = (dp, 1 - tp, cp_x)
    far = 1 - tp

    def piece_of(c):
        return c + tp * (7 - 2 * c)

    p = piece_of(cp)
    p_sib = piece_of(cp_sib)
    p_x = piece_of(cp_x)
    p_xs = piece_of(cp_xs)
    is_h = tp == 1
    is_l = tp == 0
    x_sends = xc == tp
    x_gets = xc != tp

    def load(i, src, dst):
        return pltpu.make_async_copy(src, dst, lsem.at[i])

    loads = [load(0, x_hbm, xs),
             load(1, wk_hbm, wkv_n.at[:, pl.ds(0, HD)]),
             load(2, wv_hbm, wkv_n.at[:, pl.ds(HD, HD)])]
    loads += [load(3 + j, wq_hbm.at[:, pl.ds(256 * j, 256)], wq_n.at[j]) for j in range(4)]
    loads += [load(7, wo_hbm, wo_n)]
    for cpy in loads[:3]:
        cpy.start()

    bar = pltpu.get_barrier_semaphore()
    for dev in (sib, xn, yn, dg):
        pl.semaphore_signal(bar, 1, device_id=dev, device_id_type=MESH)
    pl.semaphore_wait(bar, 4)

    def remote(src, dst, ss, rs, dev):
        return pltpu.make_async_remote_copy(src, dst, ss, rs, device_id=dev, device_id_type=MESH)

    def quarter(k, q):
        if isinstance(k, int) and k == 0:
            return [a_f.at[0, pl.ds(q * 512, 512), :]]
        if isinstance(k, int) and k < 5:
            return [a_f.at[k, pl.ds(q * 512, 512), :]]
        return [wo_f.at[k - 5, pl.ds(q * 32, 32), :]]

    def y_send(k):
        q = cp
        if isinstance(k, int) and k == 0:
            rows = pl.ds(q * 512, 512)
            return [remote(wk_hbm.at[rows, :], a_f.at[0, rows, pl.ds(0, HD)], ys.at[0], yr.at[0], yn),
                    remote(wv_hbm.at[rows, :], a_f.at[0, rows, pl.ds(HD, HD)], ys.at[13], yr.at[13], yn)]
        if isinstance(k, int) and k < 5:
            rows = pl.ds(q * 512, 512)
            return [remote(wq_hbm.at[rows, pl.ds(256 * (k - 1), 256)], a_f.at[k, rows, :], ys.at[k], yr.at[k], yn)]
        return [remote(wo_hbm.at[pl.ds((k - 5) * HD + q * 32, 32), :], wo_f.at[k - 5, pl.ds(q * 32, 32), :],
                       ys.at[k], yr.at[k], yn)]

    def x_fwd(k):
        r = quarter(k, cp)[0]
        return remote(r, r, xsnd.at[k], xr.at[k], xn)

    def x_in(k):
        r = quarter(k, cp_x)[0]
        return remote(r, r, xsnd.at[k], xr.at[k], xn)

    def d1_fwd(k):
        r = quarter(k, cp)[0]
        return remote(r, r, d1s.at[k], d1r.at[k], sib)

    def d1_in(k):
        r = quarter(k, cp_sib)[0]
        return remote(r, r, d1s.at[k], d1r.at[k], sib)

    def d2_fwd(k):
        r = quarter(k, cp_x)[0]
        return remote(r, r, d2s.at[k], d2r.at[k], sib)

    def d2_in(k):
        r = quarter(k, cp_xs)[0]
        return remote(r, r, d2s.at[k], d2r.at[k], sib)

    def start_y(k):
        for c in y_send(k):
            c.start()

    def l_send(k):
        @pl.when(is_l)
        def _():
            start_y(k)

    def relay_y(k):
        for c in y_send(k):
            c.wait_recv()
        x_fwd(k).start()
        d1_fwd(k).start()

    def relay_x(k):
        x_in(k).wait_recv()
        d2_fwd(k).start()

    def ready(k):
        d1_in(k).wait_recv()
        d2_in(k).wait_recv()

    def kv_ref(piece, e):
        return kvb.at[e, pl.ds(piece * R, R), :]

    def kv_copy(piece, e, ssem, dev):
        r = kv_ref(piece, e)
        return remote(r, r, ssem, kvr.at[piece, e], dev)

    def kv_wait(piece, e):
        kv_copy(piece, e, kvs.at[0], sib).wait_recv()

    def own_kv_sends(e, slot):
        kv_copy(p, e, kvs.at[slot], sib).start()

        @pl.when(x_sends)
        def _():
            kv_copy(p, e, kvs.at[2 + slot], xn).start()

        @pl.when(is_l)
        def _():
            kv_copy(p, e, kvs.at[4 + slot], yn).start()

    def project(w):
        return dot_nn(xs[...], w).astype(BF16)

    def kv_project(w, e):
        kvb[e, pl.ds(pl.multiple_of(p * R, R), R), :] = project(w)

    def exp_scaled(d):
        return jnp.exp2(d * EXP2_SCALE)

    def soft_new(slot, rows, s, v):
        m = jnp.max(s, axis=-1, keepdims=True)
        parts = [exp_scaled(s[:, t:t + 128] - m) for t in range(0, s.shape[1], 128)]
        m_st[slot, rows, :] = jnp.broadcast_to(m, (m.shape[0], 128))
        l_st[slot, rows, :] = functools.reduce(jnp.add, parts)
        acc_st[slot, rows, :] = dot_nn(jnp.concatenate([t.astype(BF16) for t in parts], axis=1), v)

    def soft_add(slot, s, v):
        m_old = m_st[slot]
        m_new = jnp.maximum(m_old, jnp.max(s, axis=-1, keepdims=True))
        alpha = exp_scaled(m_old - m_new)
        parts = [exp_scaled(s[:, t:t + 128] - m_new) for t in range(0, s.shape[1], 128)]
        m_st[slot] = m_new
        l_st[slot] = l_st[slot] * alpha + functools.reduce(jnp.add, parts)
        pr = jnp.concatenate([t.astype(BF16) for t in parts], axis=1)
        acc_st[slot] = acc_st[slot] * alpha + dot_nn(pr, v)

    def att_own(slot, qi, e, n, heads):
        base = pl.multiple_of((p + 1 - n) * R, R)
        k = kvb[e, pl.ds(base, n * R), 0:HD]
        v = kvb[e, pl.ds(base, n * R), HD:2 * HD]
        row = lax.broadcasted_iota(jnp.int32, (R, R), 0)
        col = lax.broadcasted_iota(jnp.int32, (R, R), 1)
        for u in range(heads):
            s = dot_nt(qb[qi + u], k)
            own = jnp.where(row >= col, s[:, (n - 1) * R:], -jnp.inf)
            if n > 1:
                own = jnp.concatenate([s[:, :(n - 1) * R], own], axis=1)
            soft_new(slot + u, slice(0, R), own, v)

    def att_tile(slot, qi, e, piece, n_pieces):
        base = pl.multiple_of(piece * R, R)
        k = kvb[e, pl.ds(base, n_pieces * R), 0:HD]
        v = kvb[e, pl.ds(base, n_pieces * R), HD:2 * HD]
        for u in range(2):
            soft_add(slot + u, dot_nt(qb[qi + u], k), v)

    def finish_head(slot, oi):
        l = jnp.sum(l_st[slot], axis=-1, keepdims=True)
        ob[oi] = (acc_st[slot] / l).astype(BF16)

    def dyn(k, fn):
        @pl.when(k < 5)
        def _():
            fn(k, lambda q: a_f.at[k, pl.ds(q * 512, 512), :])

        @pl.when(k >= 5)
        def _():
            fn(k, lambda q: wo_f.at[k - 5, pl.ds(q * 32, 32), :])

    def ry(k):
        def fn(k, at):
            r = at(cp)
            remote(r, r, ys.at[k], yr.at[k], yn).wait_recv()
            remote(r, r, xsnd.at[k], xr.at[k], xn).start()
            remote(r, r, d1s.at[k], d1r.at[k], sib).start()
        dyn(k, fn)

    def rx(k):
        def fn(k, at):
            r = at(cp_x)
            remote(r, r, xsnd.at[k], xr.at[k], xn).wait_recv()
            remote(r, r, d2s.at[k], d2r.at[k], sib).start()
        dyn(k, fn)

    start_y(0)
    for cpy in loads[3:7]:
        cpy.start()
    loads[0].wait()
    loads[1].wait()
    loads[2].wait()
    kv_project(wkv_n[...], tp)
    own_kv_sends(tp, 0)
    start_y(1)
    loads[7].start()

    def q_near(j, carry):
        load(3 + j, wq_hbm.at[:, pl.ds(pl.multiple_of(256 * j, 256), 256)], wq_n.at[j]).wait()
        r = project(wq_n[j])
        qb[2 * j] = r[:, 0:HD]
        qb[2 * j + 1] = r[:, HD:2 * HD]
        return carry

    lax.fori_loop(0, 4, q_near, 0)

    def near_self(i, carry):
        att_own(4 * i, 4 * i, tp, 1, 4)

        @pl.when(i == 0)
        def _():
            relay_y(0)

        return carry

    lax.fori_loop(0, 2, near_self, 0)

    @pl.when(x_gets)
    def _():
        kv_wait(p_x, tp)
        kv_copy(p_x, tp, kvs.at[7], sib).start()

    kv_wait(p_sib, tp)

    @pl.when(p_sib < p)
    def _():
        def body(i, carry):
            att_tile(2 * i, 2 * i, tp, p_sib, 1)
            return carry

        lax.fori_loop(0, 4, body, 0)

    @pl.when(is_h)
    def _():
        kv_wait(cp, 0)
        kv_copy(cp, 0, kvs.at[11], xn).start()
        kv_copy(cp, 0, kvs.at[9], sib).start()

    @pl.when(x_gets)
    def _():
        kv_wait(p_xs, tp)

    def near_x(i, carry):
        @pl.when(x_gets)
        def _():
            att_tile(2 * i, 2 * i, tp, lax.min(p_x, p_xs), 2)

        @pl.when(i == 0)
        def _():
            relay_x(0)

        @pl.when(i == 1)
        def _():
            ready(0)
            kv_project(a_f[0], far)
            own_kv_sends(far, 1)

        @pl.when(i == 3)
        def _():
            relay_y(1)

            @pl.when(is_h)
            def _():
                for k in range(2, 5):
                    start_y(k)

                def send_rest(k, c):
                    start_y(k)
                    return c

                lax.fori_loop(5, N_ITEMS, send_rest, 0)

        return carry

    lax.fori_loop(0, 4, near_x, 0)
    kv_wait(p_sib, far)

    @pl.when(is_h)
    def _():
        kv_wait(cp_x, 0)
        kv_copy(cp_x, 0, kvs.at[12], sib).start()
        kv_wait(cp_sib, 0)
        kv_wait(cp, 1)
        kv_copy(cp, 1, kvs.at[10], sib).start()
        kv_wait(cp_sib, 1)

    def near_l(i, carry):
        @pl.when(is_h)
        def _():
            att_tile(2 * i, 2 * i, 1, 2 * xc, 2)

        @pl.when((i == 0) & is_l)
        def _():
            kv_copy(p, far, kvs.at[5], yn).wait_send()
            kv_copy(p, far, kvs.at[6], dg).start()
            start_y(2)

        @pl.when((i == 0) & x_gets)
        def _():
            kv_wait(p_x, far)
            kv_copy(p_x, far, kvs.at[8], sib).start()

        @pl.when((i == 2) & is_h)
        def _():
            kv_wait(cp_x, 1)
            kv_copy(cp_x, 1, kvs.at[13], sib).start()

        @pl.when(i == 3)
        def _():
            l_send(3)
            relay_x(1)

        return carry

    lax.fori_loop(0, 4, near_l, 0)

    @pl.when(x_gets)
    def _():
        kv_wait(p_xs, far)

    @pl.when(is_h)
    def _():
        kv_wait(cp_xs, 0)

    def far_pair(j, carry):
        @pl.when(j == 1)
        def _():
            @pl.when(is_h)
            def _():
                kv_wait(cp_xs, 1)

            def body(i, c):
                @pl.when(is_h)
                def _():
                    att_tile(2 * i, 2 * i, 1, 2 - 2 * xc, 2)

                @pl.when(i == 1)
                def _():
                    ry(3)
                    l_send(5)
                    l_send(6)
                    rx(2)

                return c

            lax.fori_loop(0, 4, body, 0)

        @pl.when(j == 2)
        def _():
            ry(6)
            l_send(9)
            rx(4)

        @pl.when(j == 3)
        def _():
            rx(7)

        rd = a_f.at[1 + j, pl.ds(cp_sib * 512, 512), :]
        remote(rd, rd, d1s.at[1 + j], d1r.at[1 + j], sib).wait_recv()
        rd2 = a_f.at[1 + j, pl.ds(cp_xs * 512, 512), :]
        remote(rd2, rd2, d2s.at[1 + j], d2r.at[1 + j], sib).wait_recv()
        r = project(a_f[1 + j])
        qi = 8 + 2 * j
        qb[qi] = r[:, 0:HD]
        qb[qi + 1] = r[:, HD:2 * HD]
        for n in range(1, 5):
            @pl.when(p - 4 * tp + 1 == n)
            def _():
                att_own(8, qi, far, n, 2)

        @pl.when(j == 0)
        def _():
            ry(2)
            l_send(4)

        @pl.when(j == 1)
        def _():
            ry(4)
            l_send(7)
            rx(3)

        @pl.when(j == 2)
        def _():
            ry(7)
            l_send(10)
            rx(5)

        @pl.when(j == 3)
        def _():
            ry(9)
            l_send(12)
            rx(8)

        @pl.when(is_h)
        def _():
            att_tile(8, qi, far, 0, 4)

        @pl.when(j == 1)
        def _():
            ry(5)
            l_send(8)

        @pl.when(j == 2)
        def _():
            rx(6)
            ry(8)
            l_send(11)

        @pl.when(j == 3)
        def _():
            ry(10)
            rx(9)

        finish_head(8, qi)
        finish_head(9, qi + 1)
        return carry

    lax.fori_loop(0, 4, far_pair, 0)

    def near_finish(h, carry):
        finish_head(h, h)
        return carry

    lax.fori_loop(0, 8, near_finish, 0)
    relay_y(11)
    relay_x(10)

    loads[7].wait()
    for k in range(4):
        ready(5 + k)

    def out_first(t, carry):
        cols = pl.ds(pl.multiple_of(t * 256, 256), 256)
        o_all = jnp.concatenate([ob[i] for i in range(12)], axis=1)
        w = jnp.concatenate([wo_n[:, cols]] + [wo_f[k, :, cols] for k in range(4)], axis=0)
        yacc[:, cols] = dot_nn(o_all, w)

        @pl.when(t == 3)
        def _():
            relay_y(12)
            relay_x(11)

        return carry

    lax.fori_loop(0, 8, out_first, 0)
    relay_x(12)
    for k in range(4, 8):
        ready(5 + k)

    def out_last(t, carry):
        cols = pl.ds(pl.multiple_of(t * 512, 512), 512)
        o_last = jnp.concatenate([ob[12 + k] for k in range(4)], axis=1)
        w = jnp.concatenate([wo_f[4 + k, :, cols] for k in range(4)], axis=0)
        out_ref[:, cols] = (yacc[:, cols] + dot_nn(o_last, w)).astype(BF16)
        return carry

    lax.fori_loop(0, 4, out_last, 0)

    for k in range(5):
        for c in y_send(k):
            c.wait_send()
        x_fwd(k).wait_send()
        d1_fwd(k).wait_send()
        d2_fwd(k).wait_send()

    def drain(k, carry):
        for c in y_send(k):
            c.wait_send()
        x_fwd(k).wait_send()
        d1_fwd(k).wait_send()
        d2_fwd(k).wait_send()
        return carry

    lax.fori_loop(5, N_ITEMS, drain, 0)

    def sent(piece, e, slot, dev):
        kv_copy(piece, e, kvs.at[slot], dev).wait_send()

    sent(p, tp, 0, sib)
    sent(p, far, 1, sib)

    @pl.when(x_sends)
    def _():
        sent(p, tp, 2, xn)
        sent(p, far, 3, xn)

    @pl.when(x_gets)
    def _():
        sent(p_x, tp, 7, sib)
        sent(p_x, far, 8, sib)

    @pl.when(is_l)
    def _():
        sent(p, tp, 4, yn)
        sent(p, far, 6, dg)

    @pl.when(is_h)
    def _():
        sent(cp, 0, 9, sib)
        sent(cp, 1, 10, sib)
        sent(cp, 0, 11, xn)
        sent(cp_x, 0, 12, sib)
        sent(cp_x, 1, 13, sib)


def solution(mesh):
    row_spec = P(("dp", "cp", "tp"), None)

    def local_layer(x_loc, w_q, w_k, w_v, w_o):
        anyspec = pl.BlockSpec(memory_space=pl.ANY)
        dma = pltpu.SemaphoreType.DMA
        return pl.pallas_call(
            kernel,
            out_shape=pltpu.VMEM((R, 2048), BF16),
            in_specs=[anyspec] * 5,
            out_specs=pl.BlockSpec(memory_space=pltpu.VMEM),
            scratch_shapes=[
                pltpu.VMEM((R, 2048), BF16),
                pltpu.VMEM((2048, 256), BF16),
                pltpu.VMEM((4, 2048, 256), BF16),
                pltpu.VMEM((1024, 2048), BF16),
                pltpu.VMEM((5, 2048, 256), BF16),
                pltpu.VMEM((8, 128, 2048), BF16),
                pltpu.VMEM((2, 4096, 256), BF16),
                pltpu.VMEM((16, R, HD), BF16),
                pltpu.VMEM((16, R, HD), BF16),
                pltpu.VMEM((10, R, 128), F32),
                pltpu.VMEM((10, R, 128), F32),
                pltpu.VMEM((10, R, 128), F32),
                pltpu.VMEM((R, 2048), F32),
                dma((8,)),
                dma((14,)), dma((14,)),
                dma((13,)), dma((13,)),
                dma((13,)), dma((13,)),
                dma((13,)), dma((13,)),
                dma((8, 2)), dma((14,)),
            ],
            compiler_params=pltpu.CompilerParams(
                collective_id=0, has_side_effects=True, vmem_limit_bytes=58 * 1024 * 1024),
            name="attn_all",
        )(x_loc, w_q, w_k, w_v, w_o)

    return jax.shard_map(local_layer, mesh=mesh,
                         in_specs=(row_spec, P(None, "tp"), P(None, "tp"), P(None, "tp"), P("tp", None)),
                         out_specs=row_spec, check_vma=False)
```

```python
import functools

import jax
import jax.numpy as jnp
from jax import lax
from jax.experimental import pallas as pl
from jax.experimental.pallas import tpu as pltpu
from jax.sharding import PartitionSpec as P

HD = 128
R = 512
MESH = pl.DeviceIdType.MESH
F32 = jnp.float32
BF16 = jnp.bfloat16
EXP2_SCALE = (HD ** -0.5) * 1.4426950408889634
N_ITEMS = 13


def dot_nt(a, b):
    return lax.dot_general(a, b, (((1,), (1,)), ((), ())), preferred_element_type=F32)


def dot_nn(a, b):
    return jnp.dot(a, b, preferred_element_type=F32)


def kernel(x_hbm, wq_hbm, wk_hbm, wv_hbm, wo_hbm, out_ref,
           xs, wkv_n, wq_n, wo_n, a_f, wo_f, kvb, qb, ob, m_st, l_st, acc_st, yacc,
           lsem, ys, yr, xsnd, xr, d1s, d1r, d2s, d2r, kvr, kvs):
    dp = lax.axis_index("dp")
    tp = lax.axis_index("tp")
    cp = lax.axis_index("cp")
    xc = cp // 2
    core = cp % 2
    cp_sib = cp + 1 - 2 * core
    cp_x = (cp + 2) % 4
    cp_xs = (cp_sib + 2) % 4
    sib = (dp, tp, cp_sib)
    xn = (dp, tp, cp_x)
    yn = (dp, 1 - tp, cp)
    far = 1 - tp

    def piece_of(c):
        return c + tp * (7 - 2 * c)

    p = piece_of(cp)
    p_sib = piece_of(cp_sib)
    p_x = piece_of(cp_x)
    p_xs = piece_of(cp_xs)
    is_h = tp == 1
    is_l = tp == 0
    x_sends = xc == tp
    x_gets = xc != tp

    def load(i, src, dst):
        return pltpu.make_async_copy(src, dst, lsem.at[i])

    loads = [load(0, x_hbm, xs),
             load(1, wk_hbm, wkv_n.at[:, pl.ds(0, HD)]),
             load(2, wv_hbm, wkv_n.at[:, pl.ds(HD, HD)])]
    loads += [load(3 + j, wq_hbm.at[:, pl.ds(256 * j, 256)], wq_n.at[j]) for j in range(4)]
    loads += [load(7, wo_hbm, wo_n)]
    for cpy in loads[:3]:
        cpy.start()

    bar = pltpu.get_barrier_semaphore()
    for dev in (sib, xn, yn):
        pl.semaphore_signal(bar, 1, device_id=dev, device_id_type=MESH)
    pl.semaphore_wait(bar, 3)

    def remote(src, dst, ss, rs, dev):
        return pltpu.make_async_remote_copy(src, dst, ss, rs, device_id=dev, device_id_type=MESH)

    def quarter(k, q):
        if isinstance(k, int) and k == 0:
            return [a_f.at[0, pl.ds(q * 512, 512), :]]
        if isinstance(k, int) and k < 5:
            return [a_f.at[k, pl.ds(q * 512, 512), :]]
        return [wo_f.at[k - 5, pl.ds(q * 32, 32), :]]

    def y_send(k):
        q = cp
        if isinstance(k, int) and k == 0:
            rows = pl.ds(q * 512, 512)
            return [remote(wk_hbm.at[rows, :], a_f.at[0, rows, pl.ds(0, HD)], ys.at[0], yr.at[0], yn),
                    remote(wv_hbm.at[rows, :], a_f.at[0, rows, pl.ds(HD, HD)], ys.at[13], yr.at[13], yn)]
        if isinstance(k, int) and k < 5:
            rows = pl.ds(q * 512, 512)
            return [remote(wq_hbm.at[rows, pl.ds(256 * (k - 1), 256)], a_f.at[k, rows, :], ys.at[k], yr.at[k], yn)]
        return [remote(wo_hbm.at[pl.ds((k - 5) * HD + q * 32, 32), :], wo_f.at[k - 5, pl.ds(q * 32, 32), :],
                       ys.at[k], yr.at[k], yn)]

    def x_fwd(k):
        r = quarter(k, cp)[0]
        return remote(r, r, xsnd.at[k], xr.at[k], xn)

    def x_in(k):
        r = quarter(k, cp_x)[0]
        return remote(r, r, xsnd.at[k], xr.at[k], xn)

    def d1_fwd(k):
        r = quarter(k, cp)[0]
        return remote(r, r, d1s.at[k], d1r.at[k], sib)

    def d1_in(k):
        r = quarter(k, cp_sib)[0]
        return remote(r, r, d1s.at[k], d1r.at[k], sib)

    def d2_fwd(k):
        r = quarter(k, cp_x)[0]
        return remote(r, r, d2s.at[k], d2r.at[k], sib)

    def d2_in(k):
        r = quarter(k, cp_xs)[0]
        return remote(r, r, d2s.at[k], d2r.at[k], sib)

    def start_y(k):
        for c in y_send(k):
            c.start()

    def send_rest():
        for k in range(2, 5):
            start_y(k)

        def body(k, carry):
            start_y(k)
            return carry

        lax.fori_loop(5, N_ITEMS, body, 0)

    def relay_y(k):
        for c in y_send(k):
            c.wait_recv()
        x_fwd(k).start()
        d1_fwd(k).start()

    def relay_x(k):
        x_in(k).wait_recv()
        d2_fwd(k).start()

    def ready(k):
        d1_in(k).wait_recv()
        d2_in(k).wait_recv()

    def kv_ref(piece, e):
        return kvb.at[e, pl.ds(piece * R, R), :]

    def kv_copy(piece, e, ssem, dev):
        r = kv_ref(piece, e)
        return remote(r, r, ssem, kvr.at[piece, e], dev)

    def kv_wait(piece, e):
        kv_copy(piece, e, kvs.at[0], sib).wait_recv()

    def own_kv_sends(e, slot):
        kv_copy(p, e, kvs.at[slot], sib).start()

        @pl.when(x_sends)
        def _():
            kv_copy(p, e, kvs.at[2 + slot], xn).start()

    def own_kv_down(e, slot):
        @pl.when(is_l)
        def _():
            kv_copy(p, e, kvs.at[4 + slot], yn).start()

    def project(w):
        return dot_nn(xs[...], w).astype(BF16)

    def kv_project(w, e):
        kvb[e, pl.ds(pl.multiple_of(p * R, R), R), :] = project(w)

    def exp_scaled(d):
        return jnp.exp2(d * EXP2_SCALE)

    def soft_new(slot, rows, s, v):
        m = jnp.max(s, axis=-1, keepdims=True)
        parts = [exp_scaled(s[:, t:t + 128] - m) for t in range(0, s.shape[1], 128)]
        m_st[slot, rows, :] = jnp.broadcast_to(m, (m.shape[0], 128))
        l_st[slot, rows, :] = functools.reduce(jnp.add, parts)
        pr = jnp.concatenate([t.astype(BF16) for t in parts], axis=1)
        acc_st[slot, rows, :] = acc_st[slot, rows, :] + dot_nn(pr, v)

    def soft_add(slot, s, v):
        m_old = m_st[slot]
        m_new = jnp.maximum(m_old, jnp.max(s, axis=-1, keepdims=True))
        alpha = exp_scaled(m_old - m_new)
        parts = [exp_scaled(s[:, t:t + 128] - m_new) for t in range(0, s.shape[1], 128)]
        m_st[slot] = m_new
        l_st[slot] = l_st[slot] * alpha + functools.reduce(jnp.add, parts)
        pr = jnp.concatenate([t.astype(BF16) for t in parts], axis=1)
        acc_st[slot] = acc_st[slot] * alpha + dot_nn(pr, v)

    def att_own(slot, qi, e, n, heads):
        base = pl.multiple_of((p + 1 - n) * R, R)
        k = kvb[e, pl.ds(base, n * R), 0:HD]
        v = kvb[e, pl.ds(base, n * R), HD:2 * HD]
        row = lax.broadcasted_iota(jnp.int32, (R, R), 0)
        col = lax.broadcasted_iota(jnp.int32, (R, R), 1)
        for u in range(heads):
            acc_st[slot + u] = jnp.zeros((R, HD), F32)
            s = dot_nt(qb[qi + u], k)
            own = jnp.where(row >= col, s[:, (n - 1) * R:], -jnp.inf)
            if n > 1:
                own = jnp.concatenate([s[:, :(n - 1) * R], own], axis=1)
            soft_new(slot + u, slice(0, R), own, v)

    def att_tile(slot, qi, e, piece, n_pieces):
        base = pl.multiple_of(piece * R, R)
        k = kvb[e, pl.ds(base, n_pieces * R), 0:HD]
        v = kvb[e, pl.ds(base, n_pieces * R), HD:2 * HD]
        for u in range(2):
            soft_add(slot + u, dot_nt(qb[qi + u], k), v)

    def finish_head(slot, oi):
        l = jnp.sum(l_st[slot], axis=-1, keepdims=True)
        ob[oi] = (acc_st[slot] / l).astype(BF16)

    def dyn(k, fn):
        @pl.when(k < 5)
        def _():
            fn(k, lambda q: a_f.at[k, pl.ds(q * 512, 512), :])

        @pl.when(k >= 5)
        def _():
            fn(k, lambda q: wo_f.at[k - 5, pl.ds(q * 32, 32), :])

    def ry(k):
        def fn(k, at):
            r = at(cp)
            remote(r, r, ys.at[k], yr.at[k], yn).wait_recv()
            remote(r, r, xsnd.at[k], xr.at[k], xn).start()
            remote(r, r, d1s.at[k], d1r.at[k], sib).start()
        dyn(k, fn)

    def rx(k):
        def fn(k, at):
            r = at(cp_x)
            remote(r, r, xsnd.at[k], xr.at[k], xn).wait_recv()
            remote(r, r, d2s.at[k], d2r.at[k], sib).start()
        dyn(k, fn)

    start_y(0)
    for cpy in loads[3:7]:
        cpy.start()
    loads[0].wait()
    loads[1].wait()
    loads[2].wait()
    kv_project(wkv_n[...], tp)
    own_kv_sends(tp, 0)
    loads[7].start()

    def q_near(j, carry):
        load(3 + j, wq_hbm.at[:, pl.ds(pl.multiple_of(256 * j, 256), 256)], wq_n.at[j]).wait()
        r = project(wq_n[j])
        qb[2 * j] = r[:, 0:HD]
        qb[2 * j + 1] = r[:, HD:2 * HD]
        return carry

    lax.fori_loop(0, 4, q_near, 0)

    def near_self(i, carry):
        att_own(4 * i, 4 * i, tp, 1, 4)

        @pl.when(i == 0)
        def _():
            relay_y(0)
            own_kv_down(tp, 0)
            start_y(1)

        return carry

    lax.fori_loop(0, 2, near_self, 0)

    @pl.when(x_gets)
    def _():
        kv_wait(p_x, tp)
        kv_copy(p_x, tp, kvs.at[7], sib).start()

    kv_wait(p_sib, tp)

    @pl.when(p_sib < p)
    def _():
        def body(i, carry):
            att_tile(2 * i, 2 * i, tp, p_sib, 1)
            return carry

        lax.fori_loop(0, 4, body, 0)

    @pl.when(is_h)
    def _():
        kv_wait(cp, 0)
        kv_copy(cp, 0, kvs.at[11], xn).start()
        kv_copy(cp, 0, kvs.at[9], sib).start()

    @pl.when(x_gets)
    def _():
        kv_wait(p_xs, tp)

    relay_x(0)

    def near_x(i, carry):
        @pl.when(x_gets)
        def _():
            att_tile(2 * i, 2 * i, tp, lax.min(p_x, p_xs), 2)

        @pl.when(i == 0)
        def _():
            ready(0)
            kv_project(a_f[0], far)
            own_kv_sends(far, 1)
            own_kv_down(far, 1)
            send_rest()

        @pl.when(i == 3)
        def _():
            relay_y(1)

        return carry

    lax.fori_loop(0, 4, near_x, 0)
    kv_wait(p_sib, far)

    @pl.when(is_h)
    def _():
        kv_wait(cp_x, 0)
        kv_copy(cp_x, 0, kvs.at[12], sib).start()
        kv_wait(cp_sib, 0)
        kv_wait(cp, 1)
        kv_copy(cp, 1, kvs.at[6], xn).start()
        kv_copy(cp, 1, kvs.at[10], sib).start()
        kv_wait(cp_sib, 1)

    def near_l(i, carry):
        @pl.when(is_h)
        def _():
            att_tile(2 * i, 2 * i, 1, 2 * xc, 2)

        @pl.when((i == 0) & x_gets)
        def _():
            kv_wait(p_x, far)
            kv_copy(p_x, far, kvs.at[8], sib).start()

        @pl.when(i == 3)
        def _():
            relay_x(1)
            relay_y(2)

        return carry

    lax.fori_loop(0, 4, near_l, 0)

    @pl.when(x_gets)
    def _():
        kv_wait(p_xs, far)

    @pl.when(is_h)
    def _():
        kv_wait(cp_xs, 0)

    def events(j, table):
        for jj, evs in table.items():
            @pl.when(j == jj)
            def _():
                for kind, k in evs:
                    (ry if kind == "y" else rx)(k)

    def far_pair(j, carry):
        @pl.when(j == 1)
        def _():
            @pl.when(is_h)
            def _():
                kv_wait(cp_xs, 1)

            def body(i, c):
                @pl.when(is_h)
                def _():
                    att_tile(2 * i, 2 * i, 1, 2 - 2 * xc, 2)

                @pl.when(i == 1)
                def _():
                    ry(4)

                @pl.when(i == 3)
                def _():
                    ry(5)
                    rx(3)

                return c

            lax.fori_loop(0, 4, body, 0)

        rd = a_f.at[1 + j, pl.ds(cp_sib * 512, 512), :]
        remote(rd, rd, d1s.at[1 + j], d1r.at[1 + j], sib).wait_recv()
        rd2 = a_f.at[1 + j, pl.ds(cp_xs * 512, 512), :]
        remote(rd2, rd2, d2s.at[1 + j], d2r.at[1 + j], sib).wait_recv()
        r = project(a_f[1 + j])
        qi = 8 + 2 * j
        qb[qi] = r[:, 0:HD]
        qb[qi + 1] = r[:, HD:2 * HD]
        for n in range(1, 5):
            @pl.when(p - 4 * tp + 1 == n)
            def _():
                att_own(8, qi, far, n, 2)

        @pl.when((j == 0) & is_h)
        def _():
            kv_wait(cp_x, 1)
            kv_copy(cp_x, 1, kvs.at[13], sib).start()

        events(j, {0: [("y", 3)],
                   1: [("y", 6), ("y", 7), ("x", 4)],
                   2: [("y", 9), ("x", 6)],
                   3: [("y", 12), ("x", 8), ("x", 9)]})

        @pl.when(is_h)
        def _():
            att_tile(8, qi, far, 0, 4)

        events(j, {0: [("x", 2)],
                   1: [("y", 8), ("x", 5)],
                   2: [("y", 10), ("y", 11), ("x", 7)],
                   3: [("x", 10)]})
        finish_head(8, qi)
        finish_head(9, qi + 1)
        return carry

    lax.fori_loop(0, 4, far_pair, 0)

    def near_finish(h, carry):
        finish_head(h, h)
        return carry

    lax.fori_loop(0, 8, near_finish, 0)

    loads[7].wait()
    for k in range(4):
        ready(5 + k)

    def out_first(t, carry):
        cols = pl.ds(pl.multiple_of(t * 256, 256), 256)
        o_all = jnp.concatenate([ob[i] for i in range(12)], axis=1)
        w = jnp.concatenate([wo_n[:, cols]] + [wo_f[k, :, cols] for k in range(4)], axis=0)
        yacc[:, cols] = dot_nn(o_all, w)

        @pl.when(t == 0)
        def _():
            relay_x(11)

        @pl.when(t == 5)
        def _():
            relay_x(12)

        return carry

    lax.fori_loop(0, 8, out_first, 0)
    for k in range(4, 8):
        ready(5 + k)

    def out_last(t, carry):
        cols = pl.ds(pl.multiple_of(t * 512, 512), 512)
        o_last = jnp.concatenate([ob[12 + k] for k in range(4)], axis=1)
        w = jnp.concatenate([wo_f[4 + k, :, cols] for k in range(4)], axis=0)
        out_ref[:, cols] = (yacc[:, cols] + dot_nn(o_last, w)).astype(BF16)
        return carry

    lax.fori_loop(0, 4, out_last, 0)

    for k in range(5):
        for c in y_send(k):
            c.wait_send()
        x_fwd(k).wait_send()
        d1_fwd(k).wait_send()
        d2_fwd(k).wait_send()

    def drain(k, carry):
        for c in y_send(k):
            c.wait_send()
        x_fwd(k).wait_send()
        d1_fwd(k).wait_send()
        d2_fwd(k).wait_send()
        return carry

    lax.fori_loop(5, N_ITEMS, drain, 0)

    def sent(piece, e, slot, dev):
        kv_copy(piece, e, kvs.at[slot], dev).wait_send()

    sent(p, tp, 0, sib)
    sent(p, far, 1, sib)

    @pl.when(x_sends)
    def _():
        sent(p, tp, 2, xn)
        sent(p, far, 3, xn)

    @pl.when(x_gets)
    def _():
        sent(p_x, tp, 7, sib)
        sent(p_x, far, 8, sib)

    @pl.when(is_l)
    def _():
        sent(p, tp, 4, yn)
        sent(p, far, 5, yn)

    @pl.when(is_h)
    def _():
        sent(cp, 0, 9, sib)
        sent(cp, 1, 10, sib)
        sent(cp, 0, 11, xn)
        sent(cp, 1, 6, xn)
        sent(cp_x, 0, 12, sib)
        sent(cp_x, 1, 13, sib)


def solution(mesh):
    row_spec = P(("dp", "cp", "tp"), None)

    def local_layer(x_loc, w_q, w_k, w_v, w_o):
        anyspec = pl.BlockSpec(memory_space=pl.ANY)
        dma = pltpu.SemaphoreType.DMA
        return pl.pallas_call(
            kernel,
            out_shape=pltpu.VMEM((R, 2048), BF16),
            in_specs=[anyspec] * 5,
            out_specs=pl.BlockSpec(memory_space=pltpu.VMEM),
            scratch_shapes=[
                pltpu.VMEM((R, 2048), BF16),
                pltpu.VMEM((2048, 256), BF16),
                pltpu.VMEM((4, 2048, 256), BF16),
                pltpu.VMEM((1024, 2048), BF16),
                pltpu.VMEM((5, 2048, 256), BF16),
                pltpu.VMEM((8, 128, 2048), BF16),
                pltpu.VMEM((2, 4096, 256), BF16),
                pltpu.VMEM((16, R, HD), BF16),
                pltpu.VMEM((16, R, HD), BF16),
                pltpu.VMEM((10, R, 128), F32),
                pltpu.VMEM((10, R, 128), F32),
                pltpu.VMEM((10, R, 128), F32),
                pltpu.VMEM((R, 2048), F32),
                dma((8,)),
                dma((14,)), dma((14,)),
                dma((13,)), dma((13,)),
                dma((13,)), dma((13,)),
                dma((13,)), dma((13,)),
                dma((8, 2)), dma((14,)),
            ],
            compiler_params=pltpu.CompilerParams(
                collective_id=0, has_side_effects=True, vmem_limit_bytes=58 * 1024 * 1024),
            name="attn_all",
        )(x_loc, w_q, w_k, w_v, w_o)

    return jax.shard_map(local_layer, mesh=mesh,
                         in_specs=(row_spec, P(None, "tp"), P(None, "tp"), P(None, "tp"), P("tp", None)),
                         out_specs=row_spec, check_vma=False)
```

```python
import functools

import jax
import jax.numpy as jnp
from jax import lax
from jax.experimental import pallas as pl
from jax.experimental.pallas import tpu as pltpu
from jax.sharding import PartitionSpec as P

HD = 128
R = 512
MESH = pl.DeviceIdType.MESH
F32 = jnp.float32
BF16 = jnp.bfloat16
EXP2_SCALE = (HD ** -0.5) * 1.4426950408889634
N_ITEMS = 13


def dot_nt(a, b):
    return lax.dot_general(a, b, (((1,), (1,)), ((), ())), preferred_element_type=F32)


def dot_nn(a, b):
    return jnp.dot(a, b, preferred_element_type=F32)


def kernel(x_hbm, wq_hbm, wk_hbm, wv_hbm, wo_hbm, out_ref,
           xs, wkv_n, wq_n, wo_n, a_f, wo_f, kvb, qb, ob, m_st, l_st, acc_st, yacc,
           lsem, ys, yr, xsnd, xr, d1s, d1r, d2s, d2r, kvr, kvs):
    dp = lax.axis_index("dp")
    tp = lax.axis_index("tp")
    cp = lax.axis_index("cp")
    xc = cp // 2
    core = cp % 2
    cp_sib = cp + 1 - 2 * core
    cp_x = (cp + 2) % 4
    cp_xs = (cp_sib + 2) % 4
    sib = (dp, tp, cp_sib)
    xn = (dp, tp, cp_x)
    yn = (dp, 1 - tp, cp)
    far = 1 - tp

    def piece_of(c):
        return c + tp * (7 - 2 * c)

    p = piece_of(cp)
    p_sib = piece_of(cp_sib)
    p_x = piece_of(cp_x)
    p_xs = piece_of(cp_xs)
    is_h = tp == 1
    is_l = tp == 0
    x_sends = xc == tp
    x_gets = xc != tp

    def load(i, src, dst):
        return pltpu.make_async_copy(src, dst, lsem.at[i])

    loads = [load(0, x_hbm, xs),
             load(1, wk_hbm, wkv_n.at[:, pl.ds(0, HD)]),
             load(2, wv_hbm, wkv_n.at[:, pl.ds(HD, HD)])]
    loads += [load(3 + j, wq_hbm.at[:, pl.ds(256 * j, 256)], wq_n.at[j]) for j in range(4)]
    loads += [load(7, wo_hbm, wo_n)]
    for cpy in loads[:3]:
        cpy.start()

    bar = pltpu.get_barrier_semaphore()
    for dev in (sib, xn, yn):
        pl.semaphore_signal(bar, 1, device_id=dev, device_id_type=MESH)
    pl.semaphore_wait(bar, 3)

    def remote(src, dst, ss, rs, dev):
        return pltpu.make_async_remote_copy(src, dst, ss, rs, device_id=dev, device_id_type=MESH)

    def quarter(k, q):
        if isinstance(k, int) and k == 0:
            return [a_f.at[0, pl.ds(q * 512, 512), :]]
        if isinstance(k, int) and k < 5:
            return [a_f.at[k, pl.ds(q * 512, 512), :]]
        return [wo_f.at[k - 5, pl.ds(q * 32, 32), :]]

    def y_send(k):
        q = cp
        if isinstance(k, int) and k == 0:
            rows = pl.ds(q * 512, 512)
            return [remote(wk_hbm.at[rows, :], a_f.at[0, rows, pl.ds(0, HD)], ys.at[0], yr.at[0], yn),
                    remote(wv_hbm.at[rows, :], a_f.at[0, rows, pl.ds(HD, HD)], ys.at[13], yr.at[13], yn)]
        if isinstance(k, int) and k < 5:
            rows = pl.ds(q * 512, 512)
            return [remote(wq_hbm.at[rows, pl.ds(256 * (k - 1), 256)], a_f.at[k, rows, :], ys.at[k], yr.at[k], yn)]
        return [remote(wo_hbm.at[pl.ds((k - 5) * HD + q * 32, 32), :], wo_f.at[k - 5, pl.ds(q * 32, 32), :],
                       ys.at[k], yr.at[k], yn)]

    def x_fwd(k):
        r = quarter(k, cp)[0]
        return remote(r, r, xsnd.at[k], xr.at[k], xn)

    def x_in(k):
        r = quarter(k, cp_x)[0]
        return remote(r, r, xsnd.at[k], xr.at[k], xn)

    def d1_fwd(k):
        r = quarter(k, cp)[0]
        return remote(r, r, d1s.at[k], d1r.at[k], sib)

    def d1_in(k):
        r = quarter(k, cp_sib)[0]
        return remote(r, r, d1s.at[k], d1r.at[k], sib)

    def d2_fwd(k):
        r = quarter(k, cp_x)[0]
        return remote(r, r, d2s.at[k], d2r.at[k], sib)

    def d2_in(k):
        r = quarter(k, cp_xs)[0]
        return remote(r, r, d2s.at[k], d2r.at[k], sib)

    def start_y(k):
        for c in y_send(k):
            c.start()

    def send_rest():
        for k in range(2, 5):
            start_y(k)

        def body(k, carry):
            start_y(k)
            return carry

        lax.fori_loop(5, N_ITEMS, body, 0)

    def relay_y(k):
        for c in y_send(k):
            c.wait_recv()
        x_fwd(k).start()
        d1_fwd(k).start()

    def relay_x(k):
        x_in(k).wait_recv()
        d2_fwd(k).start()

    def ready(k):
        d1_in(k).wait_recv()
        d2_in(k).wait_recv()

    def kv_ref(piece, e):
        return kvb.at[e, pl.ds(piece * R, R), :]

    def kv_copy(piece, e, ssem, dev):
        r = kv_ref(piece, e)
        return remote(r, r, ssem, kvr.at[piece, e], dev)

    def kv_wait(piece, e):
        kv_copy(piece, e, kvs.at[0], sib).wait_recv()

    def own_kv_sends(e, slot):
        kv_copy(p, e, kvs.at[slot], sib).start()

        @pl.when(x_sends)
        def _():
            kv_copy(p, e, kvs.at[2 + slot], xn).start()

    def own_kv_down(e, slot):
        @pl.when(is_l)
        def _():
            kv_copy(p, e, kvs.at[4 + slot], yn).start()

    def project(w):
        return dot_nn(xs[...], w).astype(BF16)

    def kv_project(w, e):
        kvb[e, pl.ds(pl.multiple_of(p * R, R), R), :] = project(w)

    def exp_scaled(d):
        return jnp.exp2(d * EXP2_SCALE)

    def soft_new(slot, rows, s, v):
        m = jnp.max(s, axis=-1, keepdims=True)
        parts = [exp_scaled(s[:, t:t + 128] - m) for t in range(0, s.shape[1], 128)]
        m_st[slot, rows, :] = jnp.broadcast_to(m, (m.shape[0], 128))
        l_st[slot, rows, :] = functools.reduce(jnp.add, parts)
        pr = jnp.concatenate([t.astype(BF16) for t in parts], axis=1)
        acc_st[slot, rows, :] = acc_st[slot, rows, :] + dot_nn(pr, v)

    def soft_add(slot, s, v):
        m_old = m_st[slot]
        m_new = jnp.maximum(m_old, jnp.max(s, axis=-1, keepdims=True))
        alpha = exp_scaled(m_old - m_new)
        parts = [exp_scaled(s[:, t:t + 128] - m_new) for t in range(0, s.shape[1], 128)]
        m_st[slot] = m_new
        l_st[slot] = l_st[slot] * alpha + functools.reduce(jnp.add, parts)
        pr = jnp.concatenate([t.astype(BF16) for t in parts], axis=1)
        acc_st[slot] = acc_st[slot] * alpha + dot_nn(pr, v)

    def att_own(slot, qi, e, n, heads):
        base = pl.multiple_of((p + 1 - n) * R, R)
        k = kvb[e, pl.ds(base, n * R), 0:HD]
        v = kvb[e, pl.ds(base, n * R), HD:2 * HD]
        row = lax.broadcasted_iota(jnp.int32, (R, R), 0)
        col = lax.broadcasted_iota(jnp.int32, (R, R), 1)
        for u in range(heads):
            acc_st[slot + u] = jnp.zeros((R, HD), F32)
            s = dot_nt(qb[qi + u], k)
            own = jnp.where(row >= col, s[:, (n - 1) * R:], -jnp.inf)
            if n > 1:
                own = jnp.concatenate([s[:, :(n - 1) * R], own], axis=1)
            soft_new(slot + u, slice(0, R), own, v)

    def att_tile(slot, qi, e, piece, n_pieces):
        base = pl.multiple_of(piece * R, R)
        k = kvb[e, pl.ds(base, n_pieces * R), 0:HD]
        v = kvb[e, pl.ds(base, n_pieces * R), HD:2 * HD]
        for u in range(2):
            soft_add(slot + u, dot_nt(qb[qi + u], k), v)

    def finish_head(slot, oi):
        l = jnp.sum(l_st[slot], axis=-1, keepdims=True)
        ob[oi] = (acc_st[slot] / l).astype(BF16)

    def dyn(k, fn):
        @pl.when(k < 5)
        def _():
            fn(k, lambda q: a_f.at[k, pl.ds(q * 512, 512), :])

        @pl.when(k >= 5)
        def _():
            fn(k, lambda q: wo_f.at[k - 5, pl.ds(q * 32, 32), :])

    def ry(k):
        def fn(k, at):
            r = at(cp)
            remote(r, r, ys.at[k], yr.at[k], yn).wait_recv()
            remote(r, r, xsnd.at[k], xr.at[k], xn).start()
            remote(r, r, d1s.at[k], d1r.at[k], sib).start()
        dyn(k, fn)

    def rx(k):
        def fn(k, at):
            r = at(cp_x)
            remote(r, r, xsnd.at[k], xr.at[k], xn).wait_recv()
            remote(r, r, d2s.at[k], d2r.at[k], sib).start()
        dyn(k, fn)

    start_y(0)
    for cpy in loads[3:7]:
        cpy.start()
    loads[0].wait()
    loads[1].wait()
    loads[2].wait()
    kv_project(wkv_n[...], tp)
    own_kv_sends(tp, 0)
    loads[7].start()

    def q_near(j, carry):
        load(3 + j, wq_hbm.at[:, pl.ds(pl.multiple_of(256 * j, 256), 256)], wq_n.at[j]).wait()
        r = project(wq_n[j])
        qb[2 * j] = r[:, 0:HD]
        qb[2 * j + 1] = r[:, HD:2 * HD]
        return carry

    lax.fori_loop(0, 4, q_near, 0)

    def near_self(i, carry):
        att_own(4 * i, 4 * i, tp, 1, 4)

        @pl.when(i == 0)
        def _():
            relay_y(0)
            own_kv_down(tp, 0)
            start_y(1)

        return carry

    lax.fori_loop(0, 2, near_self, 0)

    @pl.when(x_gets)
    def _():
        kv_wait(p_x, tp)
        kv_copy(p_x, tp, kvs.at[7], sib).start()

    kv_wait(p_sib, tp)

    @pl.when(p_sib < p)
    def _():
        def body(i, carry):
            att_tile(2 * i, 2 * i, tp, p_sib, 1)
            return carry

        lax.fori_loop(0, 4, body, 0)

    @pl.when(is_h)
    def _():
        kv_wait(cp, 0)
        kv_copy(cp, 0, kvs.at[11], xn).start()
        kv_copy(cp, 0, kvs.at[9], sib).start()

    @pl.when(x_gets)
    def _():
        kv_wait(p_xs, tp)

    relay_x(0)

    def near_x(i, carry):
        @pl.when(x_gets)
        def _():
            att_tile(2 * i, 2 * i, tp, lax.min(p_x, p_xs), 2)

        @pl.when(i == 0)
        def _():
            ready(0)
            kv_project(a_f[0], far)
            own_kv_sends(far, 1)
            own_kv_down(far, 1)
            send_rest()

        @pl.when(i == 3)
        def _():
            relay_y(1)

        return carry

    lax.fori_loop(0, 4, near_x, 0)
    kv_wait(p_sib, far)

    @pl.when(is_h)
    def _():
        kv_wait(cp_x, 0)
        kv_copy(cp_x, 0, kvs.at[12], sib).start()
        kv_wait(cp_sib, 0)
        kv_wait(cp, 1)
        kv_copy(cp, 1, kvs.at[6], xn).start()
        kv_copy(cp, 1, kvs.at[10], sib).start()
        kv_wait(cp_sib, 1)

    def near_l(i, carry):
        @pl.when(is_h)
        def _():
            att_tile(2 * i, 2 * i, 1, 2 * xc, 2)

        @pl.when((i == 0) & x_gets)
        def _():
            kv_wait(p_x, far)
            kv_copy(p_x, far, kvs.at[8], sib).start()

        @pl.when(i == 3)
        def _():
            relay_x(1)
            relay_y(2)

        return carry

    lax.fori_loop(0, 4, near_l, 0)

    @pl.when(x_gets)
    def _():
        kv_wait(p_xs, far)

    @pl.when(is_h)
    def _():
        kv_wait(cp_xs, 0)

    def events(j, table):
        for jj, evs in table.items():
            @pl.when(j == jj)
            def _():
                for kind, k in evs:
                    (ry if kind == "y" else rx)(k)

    def far_pair(j, carry):
        @pl.when(j == 1)
        def _():
            @pl.when(is_h)
            def _():
                kv_wait(cp_xs, 1)

            def body(i, c):
                @pl.when(is_h)
                def _():
                    att_tile(2 * i, 2 * i, 1, 2 - 2 * xc, 2)

                @pl.when(i == 1)
                def _():
                    ry(4)

                @pl.when(i == 3)
                def _():
                    ry(5)
                    rx(3)

                return c

            lax.fori_loop(0, 4, body, 0)

        rd = a_f.at[1 + j, pl.ds(cp_sib * 512, 512), :]
        remote(rd, rd, d1s.at[1 + j], d1r.at[1 + j], sib).wait_recv()
        rd2 = a_f.at[1 + j, pl.ds(cp_xs * 512, 512), :]
        remote(rd2, rd2, d2s.at[1 + j], d2r.at[1 + j], sib).wait_recv()
        r = project(a_f[1 + j])
        qi = 8 + 2 * j
        qb[qi] = r[:, 0:HD]
        qb[qi + 1] = r[:, HD:2 * HD]
        for n in range(1, 5):
            @pl.when(p - 4 * tp + 1 == n)
            def _():
                att_own(8, qi, far, n, 2)

        @pl.when((j == 0) & is_h)
        def _():
            kv_wait(cp_x, 1)
            kv_copy(cp_x, 1, kvs.at[13], sib).start()

        events(j, {0: [("y", 3)],
                   1: [("y", 6), ("y", 7), ("x", 4)],
                   2: [("y", 9), ("x", 6)],
                   3: [("y", 12), ("x", 8), ("x", 9)]})

        @pl.when(is_h)
        def _():
            att_tile(8, qi, far, 0, 4)

        events(j, {0: [("x", 2)],
                   1: [("y", 8), ("x", 5)],
                   2: [("y", 10), ("y", 11), ("x", 7)],
                   3: [("x", 10)]})
        finish_head(8, qi)
        finish_head(9, qi + 1)
        return carry

    lax.fori_loop(0, 4, far_pair, 0)

    def near_finish(h, carry):
        finish_head(h, h)
        return carry

    lax.fori_loop(0, 8, near_finish, 0)

    loads[7].wait()
    for k in range(4):
        ready(5 + k)

    def out_first(t, carry):
        cols = pl.ds(pl.multiple_of(t * 256, 256), 256)
        o_all = jnp.concatenate([ob[i] for i in range(12)], axis=1)
        w = jnp.concatenate([wo_n[:, cols]] + [wo_f[k, :, cols] for k in range(4)], axis=0)
        yacc[:, cols] = dot_nn(o_all, w)

        @pl.when(t == 0)
        def _():
            relay_x(11)

        @pl.when(t == 5)
        def _():
            relay_x(12)

        return carry

    lax.fori_loop(0, 8, out_first, 0)
    for k in range(5):
        for c in y_send(k):
            c.wait_send()
        x_fwd(k).wait_send()
        d1_fwd(k).wait_send()
        d2_fwd(k).wait_send()

    def drain(k, carry):
        for c in y_send(k):
            c.wait_send()
        x_fwd(k).wait_send()
        d1_fwd(k).wait_send()
        d2_fwd(k).wait_send()
        return carry

    lax.fori_loop(5, 11, drain, 0)

    def sent(piece, e, slot, dev):
        kv_copy(piece, e, kvs.at[slot], dev).wait_send()

    sent(p, tp, 0, sib)
    sent(p, far, 1, sib)

    @pl.when(x_sends)
    def _():
        sent(p, tp, 2, xn)
        sent(p, far, 3, xn)

    @pl.when(x_gets)
    def _():
        sent(p_x, tp, 7, sib)
        sent(p_x, far, 8, sib)

    @pl.when(is_l)
    def _():
        sent(p, tp, 4, yn)
        sent(p, far, 5, yn)

    @pl.when(is_h)
    def _():
        sent(cp, 0, 9, sib)
        sent(cp, 1, 10, sib)
        sent(cp, 0, 11, xn)
        sent(cp, 1, 6, xn)
        sent(cp_x, 0, 12, sib)
        sent(cp_x, 1, 13, sib)

    for k in range(4, 8):
        ready(5 + k)

    def out_last(t, carry):
        cols = pl.ds(pl.multiple_of(t * 512, 512), 512)
        o_last = jnp.concatenate([ob[12 + k] for k in range(4)], axis=1)
        w = jnp.concatenate([wo_f[4 + k, :, cols] for k in range(4)], axis=0)
        out_ref[:, cols] = (yacc[:, cols] + dot_nn(o_last, w)).astype(BF16)
        return carry

    lax.fori_loop(0, 4, out_last, 0, unroll=True)

    lax.fori_loop(11, N_ITEMS, drain, 0)


def solution(mesh):
    row_spec = P(("dp", "cp", "tp"), None)

    def local_layer(x_loc, w_q, w_k, w_v, w_o):
        anyspec = pl.BlockSpec(memory_space=pl.ANY)
        dma = pltpu.SemaphoreType.DMA
        return pl.pallas_call(
            kernel,
            out_shape=pltpu.VMEM((R, 2048), BF16),
            in_specs=[anyspec] * 5,
            out_specs=pl.BlockSpec(memory_space=pltpu.VMEM),
            scratch_shapes=[
                pltpu.VMEM((R, 2048), BF16),
                pltpu.VMEM((2048, 256), BF16),
                pltpu.VMEM((4, 2048, 256), BF16),
                pltpu.VMEM((1024, 2048), BF16),
                pltpu.VMEM((5, 2048, 256), BF16),
                pltpu.VMEM((8, 128, 2048), BF16),
                pltpu.VMEM((2, 4096, 256), BF16),
                pltpu.VMEM((16, R, HD), BF16),
                pltpu.VMEM((16, R, HD), BF16),
                pltpu.VMEM((10, R, 128), F32),
                pltpu.VMEM((10, R, 128), F32),
                pltpu.VMEM((10, R, 128), F32),
                pltpu.VMEM((R, 2048), F32),
                dma((8,)),
                dma((14,)), dma((14,)),
                dma((13,)), dma((13,)),
                dma((13,)), dma((13,)),
                dma((13,)), dma((13,)),
                dma((8, 2)), dma((14,)),
            ],
            compiler_params=pltpu.CompilerParams(
                collective_id=0, has_side_effects=True, vmem_limit_bytes=58 * 1024 * 1024),
            name="attn_all",
        )(x_loc, w_q, w_k, w_v, w_o)

    return jax.shard_map(local_layer, mesh=mesh,
                         in_specs=(row_spec, P(None, "tp"), P(None, "tp"), P(None, "tp"), P("tp", None)),
                         out_specs=row_spec, check_vma=False)
```
